32 devices in a mesh: depth: 8 (over y, x, core), screen: 4 (over z).
Axes of the slice: x: 2, y: 2, z: 4, core: 2. Of those that a mesh axis runs over, the one named last changes fastest.
Arguments:
- block_tile: int32 [8, 8192], P('depth', 'screen'), may hold values from 0 to 127
- block_count: int32 [8, 4], P('depth', 'screen'), may hold values from 256 to 2048, as said below
- slab_rank: int32 [8], replicated, may hold values from 0 to 7, each once
- corner: int32 [2, 8, 8192, 128], P(None, 'depth', 'screen'), may hold values from 0 to 16
- offset: float32 [2, 8, 8192, 128], P(None, 'depth', 'screen'), may hold values from 0.25 to 0.75
- radius: float32 [8, 8192, 128], P('depth', 'screen'), may hold values from 3 to 8
- emission: float32 [3, 8, 8192, 128], P(None, 'depth', 'screen'), may hold values from 0.002 to 0.02
- extinction: float32 [8, 8192, 128], P('depth', 'screen'), may hold values from 0.001 to 0.01
Outputs:
- image_tiles: float32 [128, 32, 128], P(('depth', 'screen'))
The draws below stay inside these ranges and needn't reach their ends.
Inputs may be any that keep to these rules, and one draw needn't show every extreme that they name: The live slots of a device are its first block_count slots; one device of every draw has all 2048 slots live. `block_tile`: a block holds particles of one tile. `corner`: a footprint box lies inside its tile. `slab_rank`: each slab once.
All inputs are finite; a program needn't handle non-finite values.
Results may differ from the reference program's by a relative error of at most 0.0003.
Values sent between devices are 32-bit elements; how exact they have to be, the bound alone decides.
No kernel may reach another device: no remote copies, remote signals or barrier semaphores. Data moves between devices by JAX's collectives and lax.ppermute only.
A program may use at most 128 MiB of HBM per device.

```python
import math
import jax
import jax.numpy as jnp
import numpy as np
from jax import lax

TS = 32
FOOT = 16
PB = 128
BLK_DEV = 2048
TILES = 128
N_DEPTH = 8
N_SCREEN = 4


def draw_block_count(key, part):
    counts = jax.random.randint(key, (N_DEPTH, N_SCREEN), max(1, BLK_DEV // 8), BLK_DEV // 2 + 1)
    fullest = jax.random.randint(jax.random.fold_in(key, 7), (), 0, N_DEPTH * N_SCREEN)
    flattened = jnp.where(jnp.arange(N_DEPTH * N_SCREEN) == fullest, BLK_DEV, counts.reshape(-1))
    return flattened.reshape(N_DEPTH, N_SCREEN).astype(jnp.int32)


def place_ends(values, rng, low, high):
    shape = values.shape
    index_at = [jax.random.randint(jax.random.fold_in(rng, axis), (), 0, shape[axis]) for axis in range(len(shape))]
    values = values.at[tuple(index_at)].set(low)
    longest = shape.index(max(shape))
    index_at[longest] = (index_at[longest] + 1) % shape[longest]
    return values.at[tuple(index_at)].set(high)


def block_levels(rng, shape, cuts, low, high):
    factor_of = 1.0
    for axis_at, parts in cuts:
        steps = jax.random.uniform(jax.random.fold_in(jax.random.fold_in(rng, 6), axis_at), (parts,), jnp.float32, low / len(cuts), high / len(cuts))
        factor_of = factor_of * jnp.repeat(jnp.exp(steps), shape[axis_at] // parts).reshape((-1,) + (1,) * (len(shape) - 1 - axis_at))
    return factor_of


def rank_table(count, lean):
    loads = [(1 << 20) // math.isqrt(rank ** lean) + 1 for rank in range(1, count + 1)]
    scale = 1 + sum(loads) // (1 << 30)
    return np.cumsum(np.array([max(1, weight // scale) for weight in loads]))


def ranked(rng, dims, amount, slope):
    table = rank_table(amount, slope)
    pick = jax.random.randint(jax.random.fold_in(rng, 1), dims, 0, int(table[amount - 1]))
    grade = jnp.searchsorted(jnp.asarray(table, jnp.int32), pick, side="right")
    return jax.random.permutation(jax.random.fold_in(rng, 2), amount)[grade].astype(jnp.int32)


def setup_inputs(seed: int = 0) -> dict:
    seeds = jax.random.split(jax.random.key(seed), 9)
    return {
        "block_tile": place_ends(ranked(seeds[0], (N_DEPTH, N_SCREEN * BLK_DEV), TILES, 1), jax.random.fold_in(seeds[0], 3), 0, TILES - 1).astype(jnp.int32),
        "block_count": draw_block_count(jax.random.fold_in(seeds[8], 71), 0),
        "slab_rank": jax.random.permutation(seeds[2], N_DEPTH).astype(jnp.int32),
        "corner": place_ends(jax.random.randint(seeds[3], (2, N_DEPTH, N_SCREEN * BLK_DEV, PB), 0, TS - FOOT + 1), jax.random.fold_in(seeds[3], 1), 0, TS - FOOT).astype(jnp.int32),
        "offset": jnp.clip(0.25 + 0.5 * jax.random.uniform(seeds[4], (2, N_DEPTH, N_SCREEN * BLK_DEV, PB), jnp.float32) ** block_levels(seeds[4], (2, N_DEPTH, N_SCREEN * BLK_DEV, PB), ((1, 8), (2, 4)), -0.2, 0.2), 0.25, 0.75),
        "radius": jnp.clip(3.0 + 5.0 * jax.random.uniform(seeds[5], (N_DEPTH, N_SCREEN * BLK_DEV, PB), jnp.float32) ** block_levels(seeds[5], (N_DEPTH, N_SCREEN * BLK_DEV, PB), ((0, 8), (1, 4)), -0.2, 0.2), 3.0, 8.0),
        "emission": jnp.clip(jnp.exp(math.log(0.02) - 2.30258502 * jax.random.uniform(seeds[6], (3, N_DEPTH, N_SCREEN * BLK_DEV, PB), jnp.float32) ** block_levels(seeds[6], (3, N_DEPTH, N_SCREEN * BLK_DEV, PB), ((1, 8), (2, 4)), -0.2, 0.2)), 0.002, 0.02),
        "extinction": jnp.clip(jnp.exp(math.log(0.01) - 2.30258502 * jax.random.uniform(seeds[7], (N_DEPTH, N_SCREEN * BLK_DEV, PB), jnp.float32) ** block_levels(seeds[7], (N_DEPTH, N_SCREEN * BLK_DEV, PB), ((0, 8), (1, 4)), -0.2, 0.2)), 0.001, 0.01),
    }


def axis_weights(corner, offset, radius, tile_side, foot):
    pixel_index = jnp.arange(tile_side, dtype=jnp.int32)
    pixel_centre = pixel_index.astype(jnp.float32) + 0.5
    centres = corner.astype(jnp.float32) + foot * offset
    scaled = (pixel_centre - centres[..., None]) / radius[..., None]
    bump_shape = jnp.maximum(1.0 - scaled * scaled, 0.0)
    inside = (pixel_index >= corner[..., None]) & (pixel_index < corner[..., None] + foot)
    return jnp.where(inside, bump_shape * bump_shape, 0.0)


def deposit(corner, offset, radius, emission, extinction, block_live, tile_side, foot):
    across = axis_weights(corner[0], offset[0], radius, tile_side, foot)
    down_weights = axis_weights(corner[1], offset[1], radius, tile_side, foot)
    fields = jnp.concatenate([emission, extinction[None]], 0) * block_live[None, :, None]
    spread = fields[..., None] * across[None]
    deposit_out = jnp.einsum('gpy,cgpx->gycx', down_weights, spread, precision=lax.Precision.HIGHEST)
    return deposit_out.reshape(deposit_out.shape[0], tile_side, 4 * tile_side)


def composite(stacked, slab_rank):
    slab_num, tile_num, tile_side, row_width = stacked.shape
    pieces = stacked.reshape(slab_num, tile_num, tile_side, 4, row_width // 4)
    glow_part = pieces[:, :, :, :3, :]
    optical = pieces[:, :, :, 3:, :]
    before = (slab_rank[None, :] < slab_rank[:, None]).astype(jnp.float32)
    prior_depth = jnp.einsum('jk,ktyax->jtyax', before, optical, precision=lax.Precision.HIGHEST)
    lighting = jnp.sum(jnp.exp(-prior_depth) * glow_part * jnp.exp(-0.5 * optical), axis=0)
    coverage = 1.0 - jnp.exp(-jnp.sum(optical, axis=0))
    return jnp.concatenate([lighting, coverage], axis=2).reshape(tile_num, tile_side, row_width)


def reference(block_tile, block_count, slab_rank, corner, offset, radius, emission, extinction):
    group_size = min(256, BLK_DEV)
    rounds = BLK_DEV // group_size
    tile_ids = block_tile.reshape(N_DEPTH, N_SCREEN, rounds, group_size)
    corners = jnp.moveaxis(corner.reshape(2, N_DEPTH, N_SCREEN, rounds, group_size, PB), 0, 3)
    offsets = jnp.moveaxis(offset.reshape(2, N_DEPTH, N_SCREEN, rounds, group_size, PB), 0, 3)
    radii = radius.reshape(N_DEPTH, N_SCREEN, rounds, group_size, PB)
    glows = jnp.moveaxis(emission.reshape(3, N_DEPTH, N_SCREEN, rounds, group_size, PB), 0, 3)
    rates = extinction.reshape(N_DEPTH, N_SCREEN, rounds, group_size, PB)

    def one_device(running, device_inputs):
        ids_dev, live_count, corner_dev, offset_dev, radius_dev, glow_dev, rate_dev = device_inputs
        slot_live = (jnp.arange(BLK_DEV, dtype=jnp.int32) < live_count).astype(jnp.float32)
        slot_live = slot_live.reshape(rounds, group_size)

        def one_round(tile_sums, round_inputs):
            ids_now, live_now, corner_now, offset_now, radius_now, glow_now, rate_now = round_inputs
            deposit_out = deposit(corner_now, offset_now, radius_now, glow_now, rate_now, live_now, TS, FOOT)
            return tile_sums.at[ids_now].add(deposit_out), None

        tile_sums, unused = lax.scan(one_round, jnp.zeros((TILES, TS, 4 * TS), jnp.float32),
                                     (ids_dev, slot_live, corner_dev, offset_dev, radius_dev, glow_dev, rate_dev))
        return running + tile_sums, None

    def one_slab(slab_inputs):
        running, unused = lax.scan(one_device, jnp.zeros((TILES, TS, 4 * TS), jnp.float32), slab_inputs)
        return running

    slab_stack = lax.map(one_slab, (tile_ids, block_count, corners, offsets, radii, glows, rates))
    return composite(slab_stack, slab_rank)
```

```python
import functools

import jax
import jax.numpy as jnp
from jax import lax
from jax.experimental import pallas as pl
from jax.experimental.pallas import tpu as pltpu
from jax.sharding import PartitionSpec as P

TS = 32
FOOT = 16
TILE_DEV = 4
N_CHUNK = 16
UNROLL = 16


def deposit_kernel(tiles_all, slots, pb, count_ref, tile_ref, corner_hbm, offset_hbm, radius_hbm,
                   emission_hbm, extinction_hbm, out_ref,
                   corner_v, offset_v, radius_v, emission_v, extinction_v, prep, acc, sems):
    rows = slots // N_CHUNK
    live_count = count_ref[0, 0]

    def copies(chunk):
        sl = pl.ds(pl.multiple_of(chunk * rows, rows), rows)
        return [
            pltpu.make_async_copy(corner_hbm.at[:, 0, sl], corner_v.at[:, sl], sems.at[chunk, 0]),
            pltpu.make_async_copy(offset_hbm.at[:, 0, sl], offset_v.at[:, sl], sems.at[chunk, 1]),
            pltpu.make_async_copy(radius_hbm.at[0, sl], radius_v.at[sl], sems.at[chunk, 2]),
            pltpu.make_async_copy(emission_hbm.at[:, 0, sl], emission_v.at[:, sl], sems.at[chunk, 3]),
            pltpu.make_async_copy(extinction_hbm.at[0, sl], extinction_v.at[sl], sems.at[chunk, 4]),
        ]

    def start_chunk(chunk, carry):
        for copy in copies(chunk):
            copy.start()
        return carry

    lax.fori_loop(0, N_CHUNK, start_chunk, 0)

    def clear(t, carry):
        acc[t] = jnp.zeros((4 * TS, 2 * TS), jnp.float32)
        return carry

    lax.fori_loop(0, tiles_all, clear, 0)

    pixel = lax.broadcasted_iota(jnp.int32, (TS, pb), 0).astype(jnp.float32)
    half = FOOT
    low_pixel = pixel[:half]
    high_pixel = pixel[half:] - float(FOOT)

    def bump(edge, centre, h2):
        s = pixel - centre
        p = h2 - s * s
        inside = jnp.concatenate([low_pixel >= edge, high_pixel < edge], axis=0)
        p = jnp.maximum(jnp.where(inside, p, 0.0), 0.0)
        return p * p

    def split(value):
        high = value.astype(jnp.bfloat16)
        low = (value - high.astype(jnp.float32)).astype(jnp.bfloat16)
        return high, low

    def one_block(row, slot):
        def param(k):
            return prep[k, pl.ds(row, 1), :]

        h2 = param(4)
        across = bump(param(0), param(1), h2)
        down = bump(param(2), param(3), h2)
        spread = jnp.concatenate([across * param(5 + c) for c in range(4)], axis=0)
        lhs = jnp.concatenate(split(spread), axis=1)
        y_high, y_low = split(down)
        rhs = jnp.concatenate(
            [jnp.concatenate([y_high, y_high], axis=1), jnp.concatenate([y_low, y_low], axis=1)],
            axis=0)
        res = lax.dot_general(lhs, rhs, (((1,), (1,)), ((), ())),
                              preferred_element_type=jnp.float32)
        return res

    def one_chunk(chunk, carry):
        for copy in copies(chunk):
            copy.wait()
        first = pl.multiple_of(chunk * rows, rows)

        @pl.when(first < live_count)
        def _():
            sl = pl.ds(first, rows)
            for axis in range(2):
                edge = corner_v[axis, sl].astype(jnp.float32)
                prep[2 * axis] = edge
                prep[2 * axis + 1] = edge + float(FOOT) * offset_v[axis, sl] - 0.5
            h2 = radius_v[sl] * radius_v[sl]
            prep[4] = h2
            inv = 1.0 / h2
            inv = inv * inv
            slot_index = first + lax.broadcasted_iota(jnp.int32, (rows, pb), 0)
            scale = jnp.where(slot_index < live_count, inv * inv, 0.0)
            for c in range(3):
                prep[5 + c] = emission_v[c, sl] * scale
            prep[8] = extinction_v[sl] * scale
            live_here = jnp.minimum(live_count - first, rows)

            def one_group(group, inner):
                base = group * UNROLL
                results = [one_block(base + k, first + base + k) for k in range(UNROLL)]
                for k in range(UNROLL):
                    t = tile_ref[0, first + base + k]
                    acc[t] = acc[t] + results[k]
                return inner

            lax.fori_loop(0, (live_here + UNROLL - 1) // UNROLL, one_group, 0)

        return carry

    lax.fori_loop(0, N_CHUNK, one_chunk, 0)

    def finish(group, carry):
        pieces = []
        for q in range(TILE_DEV):
            tile = acc[group * TILE_DEV + q]
            pieces.append(tile[:, :TS] + tile[:, TS:])
        out_ref[group] = jnp.concatenate(pieces, axis=1)
        return carry

    lax.fori_loop(0, tiles_all // TILE_DEV, finish, 0)


def deposit(block_tile, block_count, corner, offset, radius, emission, extinction, tiles_all):
    slots, pb = radius.shape[1:]
    any_space = pl.BlockSpec(memory_space=pl.ANY)
    smem = pl.BlockSpec(memory_space=pltpu.SMEM)
    return pl.pallas_call(
        functools.partial(deposit_kernel, tiles_all, slots, pb),
        out_shape=jax.ShapeDtypeStruct((tiles_all // TILE_DEV, 4 * TS, TILE_DEV * TS), jnp.float32),
        in_specs=[smem, smem] + [any_space] * 5,
        out_specs=pl.BlockSpec(memory_space=pltpu.VMEM),
        scratch_shapes=[
            pltpu.VMEM((2, slots, pb), jnp.int32),
            pltpu.VMEM((2, slots, pb), jnp.float32),
            pltpu.VMEM((slots, pb), jnp.float32),
            pltpu.VMEM((3, slots, pb), jnp.float32),
            pltpu.VMEM((slots, pb), jnp.float32),
            pltpu.VMEM((9, slots // N_CHUNK, pb), jnp.float32),
            pltpu.VMEM((tiles_all, 4 * TS, 2 * TS), jnp.float32),
            pltpu.SemaphoreType.DMA((N_CHUNK, 5)),
        ],
        compiler_params=pltpu.CompilerParams(vmem_limit_bytes=60 * 1024 * 1024),
        name="deposit",
    )(block_count, block_tile, corner, offset, radius, emission, extinction)


def composite(stacked, slab_rank):
    slabs = stacked.shape[0]
    optical = stacked[:, 3 * TS:]
    glow = stacked[:, :3 * TS].reshape(slabs, 3, TS, TILE_DEV * TS)
    before = (slab_rank[None, :] < slab_rank[:, None]).astype(jnp.float32)
    prior = sum(before[:, k, None, None] * optical[k][None] for k in range(slabs))
    fade = jnp.exp(-prior) * jnp.exp(-0.5 * optical)
    light = jnp.sum(fade[:, None] * glow, axis=0).reshape(3 * TS, TILE_DEV * TS)
    cover = 1.0 - jnp.exp(-jnp.sum(optical, axis=0))
    image = jnp.concatenate([light, cover], axis=0)
    return image.reshape(4 * TS, TILE_DEV, TS).transpose(1, 2, 0)


def shards(block_tile, block_count, slab_rank, corner, offset, radius, emission, extinction):
    depth_size = lax.axis_size("depth")
    screen_size = lax.axis_size("screen")
    tiles_all = TILE_DEV * depth_size * screen_size
    partial = deposit(block_tile, block_count, corner, offset, radius, emission, extinction, tiles_all)
    shaped = partial.reshape(depth_size, screen_size, 4 * TS, TILE_DEV * TS)
    owned = lax.psum_scatter(shaped, "screen", scatter_dimension=1, tiled=True)
    owned = owned.reshape(depth_size, 4 * TS, TILE_DEV * TS)
    slabs = lax.all_to_all(owned, "depth", split_axis=0, concat_axis=0, tiled=True)
    return composite(slabs, slab_rank)


def solution(mesh):
    placed = (
        P("depth", "screen"),
        P("depth", "screen"),
        P(),
        P(None, "depth", "screen", None),
        P(None, "depth", "screen", None),
        P("depth", "screen", None),
        P(None, "depth", "screen", None),
        P("depth", "screen", None),
    )
    return jax.shard_map(
        shards,
        mesh=mesh,
        in_specs=placed,
        out_specs=P(("depth", "screen"), None, None),
        check_vma=False,
    )
```

```python
import functools

import jax
import jax.numpy as jnp
from jax import lax
from jax.experimental import pallas as pl
from jax.experimental.pallas import tpu as pltpu
from jax.sharding import PartitionSpec as P

TS = 32
FOOT = 16
TILE_DEV = 4
N_CHUNK = 16
UNROLL = 128
SKEW = 4


def deposit_kernel(tiles_all, slots, pb, screen_size, count_ref, place_ref, tile_ref, corner_hbm,
                   offset_hbm, radius_hbm, emission_hbm, extinction_hbm, *rest):
    outs = rest[:screen_size]
    (corner_v, offset_v, radius_v, emission_v, extinction_v, prep, acc,
     late_lhs, late_rhs, sems) = rest[screen_size:]
    rows = slots // N_CHUNK
    live_count = count_ref[0, 0]

    def copies(chunk):
        sl = pl.ds(pl.multiple_of(chunk * rows, rows), rows)
        return [
            pltpu.make_async_copy(corner_hbm.at[:, 0, sl], corner_v.at[:, sl], sems.at[chunk, 0]),
            pltpu.make_async_copy(offset_hbm.at[:, 0, sl], offset_v.at[:, sl], sems.at[chunk, 1]),
            pltpu.make_async_copy(radius_hbm.at[0, sl], radius_v.at[sl], sems.at[chunk, 2]),
            pltpu.make_async_copy(emission_hbm.at[:, 0, sl], emission_v.at[:, sl], sems.at[chunk, 3]),
            pltpu.make_async_copy(extinction_hbm.at[0, sl], extinction_v.at[sl], sems.at[chunk, 4]),
        ]

    def start_chunk(chunk, carry):
        for copy in copies(chunk):
            copy.start()
        return carry

    lax.fori_loop(0, 2, start_chunk, 0)

    def clear(t, carry):
        acc[t] = jnp.zeros((4 * TS, 2 * TS), jnp.float32)
        return carry

    lax.fori_loop(0, tiles_all, clear, 0)

    pixel = lax.broadcasted_iota(jnp.int32, (TS, pb), 0).astype(jnp.float32)
    half = FOOT
    low_pixel = pixel[:half]
    high_pixel = pixel[half:] - float(FOOT)

    def bump(edge, centre, h2):
        s = pixel - centre
        p = h2 - s * s
        inside = jnp.concatenate([low_pixel >= edge, high_pixel < edge], axis=0)
        p = jnp.maximum(jnp.where(inside, p, 0.0), 0.0)
        return p * p

    def with_rest(value):
        return value, value - value.astype(jnp.bfloat16).astype(jnp.float32)

    def factors(row):
        def param(k):
            return prep[k, pl.ds(row, 1), :]

        h2 = param(4)
        across = bump(param(0), param(1), h2)
        down = bump(param(2), param(3), h2)
        spread = jnp.concatenate([across * param(5 + c) for c in range(4)], axis=0)
        lhs = jnp.concatenate(with_rest(spread), axis=1)
        rhs = jnp.concatenate(
            [jnp.concatenate([part, part], axis=1) for part in with_rest(down)], axis=0)
        return lhs, rhs

    def product(lhs, rhs):
        return lax.dot_general(lhs, rhs, (((1,), (1,)), ((), ())),
                               preferred_element_type=jnp.float32)

    def add_late(base):
        for k in range(SKEW):
            t = tile_ref[0, jnp.maximum(base - SKEW + k, 0)]
            acc[t] = acc[t] + product(late_lhs[k], late_rhs[k])

    for k in range(SKEW):
        late_lhs[k] = jnp.zeros(late_lhs.shape[1:], jnp.float32)
        late_rhs[k] = jnp.zeros(late_rhs.shape[1:], jnp.float32)

    def one_chunk(chunk, carry):
        for copy in copies(chunk):
            copy.wait()

        @pl.when(chunk + 2 < N_CHUNK)
        def _():
            start_chunk(chunk + 2, 0)

        first = pl.multiple_of(chunk * rows, rows)

        @pl.when(first < live_count)
        def _():
            sl = pl.ds(first, rows)
            for axis in range(2):
                edge = corner_v[axis, sl].astype(jnp.float32)
                prep[2 * axis] = edge
                prep[2 * axis + 1] = edge + float(FOOT) * offset_v[axis, sl] - 0.5
            h2 = radius_v[sl] * radius_v[sl]
            prep[4] = h2
            inv = 1.0 / h2
            inv = inv * inv
            slot_index = first + lax.broadcasted_iota(jnp.int32, (rows, pb), 0)
            scale = jnp.where(slot_index < live_count, inv * inv, 0.0)
            for c in range(3):
                prep[5 + c] = emission_v[c, sl] * scale
            prep[8] = extinction_v[sl] * scale
            live_here = jnp.minimum(live_count - first, rows)

            def one_group(group, inner):
                base = group * UNROLL
                late = [product(late_lhs[k], late_rhs[k]) for k in range(SKEW)]
                pairs = [factors(base + k) for k in range(UNROLL)]
                results = [product(*pair) for pair in pairs[:UNROLL - SKEW]]
                for k in range(SKEW):
                    late_lhs[k], late_rhs[k] = pairs[UNROLL - SKEW + k]
                for k, res in enumerate(late + results):
                    t = tile_ref[0, jnp.maximum(first + base - SKEW + k, 0)]
                    acc[t] = acc[t] + res
                return inner

            lax.fori_loop(0, (live_here + UNROLL - 1) // UNROLL, one_group, 0)

        return carry

    lax.fori_loop(0, N_CHUNK, one_chunk, 0)

    add_late((live_count + UNROLL - 1) // UNROLL * UNROLL)

    lane = lax.broadcasted_iota(jnp.int32, (4 * TS, TILE_DEV * TS), 1)
    even = (lane // TS) % 2 == 0

    def finish(d, carry):
        for k in range(screen_size):
            s = lax.rem(place_ref[0, 0] + k, screen_size)
            tile = (d * screen_size + s) * TILE_DEV
            wide = [jnp.concatenate([acc[tile + q], acc[tile + q + 2]], axis=1) for q in range(2)]
            turned = [pltpu.roll(wide[0], 3 * TS, axis=1), pltpu.roll(wide[1], TS, axis=1)]
            outs[k][d] = jnp.where(even, wide[0] + turned[0], wide[1] + turned[1])
        return carry

    lax.fori_loop(0, tiles_all // (TILE_DEV * screen_size), finish, 0)


def deposit(block_tile, block_count, corner, offset, radius, emission, extinction, tiles_all,
            place, screen_size):
    slots, pb = radius.shape[1:]
    any_space = pl.BlockSpec(memory_space=pl.ANY)
    smem = pl.BlockSpec(memory_space=pltpu.SMEM)
    return pl.pallas_call(
        functools.partial(deposit_kernel, tiles_all, slots, pb, screen_size),
        out_shape=[jax.ShapeDtypeStruct(
            (tiles_all // (TILE_DEV * screen_size), 4 * TS, TILE_DEV * TS), jnp.float32)
        ] * screen_size,
        in_specs=[smem, smem, smem] + [any_space] * 5,
        out_specs=[pl.BlockSpec(memory_space=pltpu.VMEM)] * screen_size,
        scratch_shapes=[
            pltpu.VMEM((2, slots, pb), jnp.int32),
            pltpu.VMEM((2, slots, pb), jnp.float32),
            pltpu.VMEM((slots, pb), jnp.float32),
            pltpu.VMEM((3, slots, pb), jnp.float32),
            pltpu.VMEM((slots, pb), jnp.float32),
            pltpu.VMEM((9, slots // N_CHUNK, pb), jnp.float32),
            pltpu.VMEM((tiles_all, 4 * TS, 2 * TS), jnp.float32),
            pltpu.VMEM((SKEW, 4 * TS, 2 * pb), jnp.float32),
            pltpu.VMEM((SKEW, 2 * TS, 2 * pb), jnp.float32),
            pltpu.SemaphoreType.DMA((N_CHUNK, 5)),
        ],
        compiler_params=pltpu.CompilerParams(vmem_limit_bytes=60 * 1024 * 1024),
        name="deposit",
    )(block_count, place, block_tile, corner, offset, radius, emission, extinction)


def composite(stacked, slab_rank):
    slabs = stacked.shape[0]
    optical = stacked[:, 3 * TS:]
    glow = stacked[:, :3 * TS].reshape(slabs, 3, TS, TILE_DEV * TS)
    before = (slab_rank[None, :] < slab_rank[:, None]).astype(jnp.float32)
    prior = sum(before[:, k, None, None] * optical[k][None] for k in range(slabs))
    fade = jnp.exp(-prior) * jnp.exp(-0.5 * optical)
    light = jnp.sum(fade[:, None] * glow, axis=0).reshape(3 * TS, TILE_DEV * TS)
    cover = 1.0 - jnp.exp(-jnp.sum(optical, axis=0))
    image = jnp.concatenate([light, cover], axis=0)
    return image.reshape(4 * TS, TILE_DEV, TS).transpose(1, 2, 0)


def shards(block_tile, block_count, slab_rank, corner, offset, radius, emission, extinction):
    depth_size = lax.axis_size("depth")
    screen_size = lax.axis_size("screen")
    tiles_all = TILE_DEV * depth_size * screen_size
    me = lax.axis_index("screen")
    partial = deposit(block_tile, block_count, corner, offset, radius, emission, extinction,
                      tiles_all, me.astype(jnp.int32).reshape(1, 1), screen_size)
    owned = partial[0]
    moved = [
        lax.ppermute(partial[k], "screen", [(i, (i + k) % screen_size) for i in range(screen_size)])
        for k in range(1, screen_size)
    ]
    for block in moved:
        owned = owned + block
    dme = lax.axis_index("depth")
    pieces = [lax.dynamic_index_in_dim(owned, dme, 0, keepdims=True)]
    for k in range(1, depth_size):
        block = lax.dynamic_index_in_dim(owned, dme ^ k, 0, keepdims=True)
        pieces.append(lax.ppermute(block, "depth", [(i, i ^ k) for i in range(depth_size)]))
    slabs = jnp.concatenate(pieces, axis=0)
    slab_rank = slab_rank[dme ^ jnp.arange(depth_size)]
    return composite(slabs, slab_rank)


def solution(mesh):
    placed = (
        P("depth", "screen"),
        P("depth", "screen"),
        P(),
        P(None, "depth", "screen", None),
        P(None, "depth", "screen", None),
        P("depth", "screen", None),
        P(None, "depth", "screen", None),
        P("depth", "screen", None),
    )
    return jax.shard_map(
        shards,
        mesh=mesh,
        in_specs=placed,
        out_specs=P(("depth", "screen"), None, None),
        check_vma=False,
    )
```

```python
import functools

import jax
import jax.numpy as jnp
from jax import lax
from jax.experimental import pallas as pl
from jax.experimental.pallas import tpu as pltpu
from jax.sharding import PartitionSpec as P

TS = 32
FOOT = 16
TILE_DEV = 4
N_CHUNK = 16
UNROLL = 128
SKEW = 4


def deposit_kernel(tiles_all, slots, pb, screen_size, count_ref, place_ref, tile_hbm, corner_hbm,
                   offset_hbm, radius_hbm, emission_hbm, extinction_hbm, *rest):
    outs = rest[:screen_size]
    (corner_v, offset_v, radius_v, emission_v, extinction_v, prep, acc,
     late_lhs, late_rhs, tile_ref, ready, sems, tile_sem, out_sems) = rest[screen_size:]
    rows = slots // N_CHUNK
    live_count = count_ref[0, 0]

    def copies(chunk):
        sl = pl.ds(pl.multiple_of(chunk * rows, rows), rows)
        return [
            pltpu.make_async_copy(corner_hbm.at[:, 0, sl], corner_v.at[:, sl], sems.at[chunk, 0]),
            pltpu.make_async_copy(offset_hbm.at[:, 0, sl], offset_v.at[:, sl], sems.at[chunk, 1]),
            pltpu.make_async_copy(radius_hbm.at[0, sl], radius_v.at[sl], sems.at[chunk, 2]),
            pltpu.make_async_copy(emission_hbm.at[:, 0, sl], emission_v.at[:, sl], sems.at[chunk, 3]),
            pltpu.make_async_copy(extinction_hbm.at[0, sl], extinction_v.at[sl], sems.at[chunk, 4]),
        ]

    def start_chunk(chunk, carry):
        for copy in copies(chunk):
            copy.start()
        return carry

    lax.fori_loop(0, 2, start_chunk, 0)
    tile_copy = pltpu.make_async_copy(tile_hbm, tile_ref, tile_sem)
    tile_copy.start()

    def clear(t, carry):
        acc[t] = jnp.zeros((4 * TS, 2 * TS), jnp.float32)
        return carry

    lax.fori_loop(0, tiles_all, clear, 0)

    quarter = TS // 4
    pixel = lax.broadcasted_iota(jnp.int32, (quarter, pb), 0).astype(jnp.float32)
    second_quarter = (pixel + float(quarter)) / float(FOOT)

    def bump(edge, centre, h2):
        s = second_quarter - centre
        p1 = h2 - s * s
        shared = p1 - 0.25
        p0 = shared + s
        p2 = shared - s
        p3 = (p2 - s) - 0.75
        inside = (pixel >= edge, pixel + float(quarter) >= edge,
                  pixel < edge, pixel + float(quarter) < edge)
        parts = [jnp.maximum(jnp.where(ok, p, 0.0), 0.0) for ok, p in zip(inside, (p0, p1, p2, p3))]
        return jnp.concatenate([p * p for p in parts], axis=0)

    def with_rest(value):
        return value, value - value.astype(jnp.bfloat16).astype(jnp.float32)

    def factors(row):
        def param(k):
            return prep[k, pl.ds(row, 1), :]

        h2 = param(4)
        across = bump(param(0), param(1), h2)
        down = bump(param(2), param(3), h2)
        spread = jnp.concatenate([across * param(5 + c) for c in range(4)], axis=0)
        lhs = jnp.concatenate(with_rest(spread), axis=1)
        rhs = jnp.concatenate(
            [jnp.concatenate([part, part], axis=1) for part in with_rest(down)], axis=0)
        return lhs, rhs

    def product(lhs, rhs):
        return lax.dot_general(lhs, rhs, (((1,), (1,)), ((), ())),
                               preferred_element_type=jnp.float32)

    def add_late(base):
        for k in range(SKEW):
            t = tile_ref[0, jnp.maximum(base - SKEW + k, 0)]
            acc[t] = acc[t] + product(late_lhs[k], late_rhs[k])

    for k in range(SKEW):
        late_lhs[k] = jnp.zeros(late_lhs.shape[1:], jnp.float32)
        late_rhs[k] = jnp.zeros(late_rhs.shape[1:], jnp.float32)

    tile_copy.wait()

    def one_chunk(chunk, carry):
        for copy in copies(chunk):
            copy.wait()

        @pl.when(chunk + 2 < N_CHUNK)
        def _():
            start_chunk(chunk + 2, 0)

        first = pl.multiple_of(chunk * rows, rows)

        @pl.when(first < live_count)
        def _():
            sl = pl.ds(first, rows)
            for axis in range(2):
                edge = corner_v[axis, sl].astype(jnp.float32)
                prep[2 * axis] = edge
                prep[2 * axis + 1] = (edge - 0.5) / float(FOOT) + offset_v[axis, sl]
            unit_radius = radius_v[sl] / float(FOOT)
            h2 = unit_radius * unit_radius
            prep[4] = h2
            inv = 1.0 / h2
            inv = inv * inv
            slot_index = first + lax.broadcasted_iota(jnp.int32, (rows, pb), 0)
            scale = jnp.where(slot_index < live_count, inv * inv, 0.0)
            for c in range(3):
                prep[5 + c] = emission_v[c, sl] * scale
            prep[8] = extinction_v[sl] * scale
            live_here = jnp.minimum(live_count - first, rows)

            def one_group(group, inner):
                base = group * UNROLL
                late = [product(late_lhs[k], late_rhs[k]) for k in range(SKEW)]
                pairs = [factors(base + k) for k in range(UNROLL)]
                results = [product(*pair) for pair in pairs[:UNROLL - SKEW]]
                for k in range(SKEW):
                    late_lhs[k], late_rhs[k] = pairs[UNROLL - SKEW + k]
                for k, res in enumerate(late + results):
                    t = tile_ref[0, jnp.maximum(first + base - SKEW + k, 0)]
                    acc[t] = acc[t] + res
                return inner

            lax.fori_loop(0, (live_here + UNROLL - 1) // UNROLL, one_group, 0)

        return carry

    lax.fori_loop(0, N_CHUNK, one_chunk, 0)

    add_late((live_count + UNROLL - 1) // UNROLL * UNROLL)

    lane = lax.broadcasted_iota(jnp.int32, (4 * TS, TILE_DEV * TS), 1)
    even = (lane // TS) % 2 == 0

    def out_copy(k, d):
        return pltpu.make_async_copy(ready.at[k, d], outs[k].at[d], out_sems.at[k, d])

    def finish(d, carry):
        for k in range(screen_size):
            s = lax.rem(place_ref[0, 0] + k, screen_size)
            tile = (d * screen_size + s) * TILE_DEV
            wide = [jnp.concatenate([acc[tile + q], acc[tile + q + 2]], axis=1) for q in range(2)]
            turned = [pltpu.roll(wide[0], 3 * TS, axis=1), pltpu.roll(wide[1], TS, axis=1)]
            ready[k, d] = jnp.where(even, wide[0] + turned[0], wide[1] + turned[1])
            out_copy(k, d).start()
        return carry

    lax.fori_loop(0, tiles_all // (TILE_DEV * screen_size), finish, 0)

    def drain(d, carry):
        for k in range(screen_size):
            out_copy(k, d).wait()
        return carry

    lax.fori_loop(0, tiles_all // (TILE_DEV * screen_size), drain, 0)


def deposit(block_tile, block_count, corner, offset, radius, emission, extinction, tiles_all,
            place, screen_size):
    slots, pb = radius.shape[1:]
    any_space = pl.BlockSpec(memory_space=pl.ANY)
    smem = pl.BlockSpec(memory_space=pltpu.SMEM)
    return pl.pallas_call(
        functools.partial(deposit_kernel, tiles_all, slots, pb, screen_size),
        out_shape=[jax.ShapeDtypeStruct(
            (tiles_all // (TILE_DEV * screen_size), 4 * TS, TILE_DEV * TS), jnp.float32)
        ] * screen_size,
        in_specs=[smem, smem] + [any_space] * 6,
        out_specs=[any_space] * screen_size,
        scratch_shapes=[
            pltpu.VMEM((2, slots, pb), jnp.int32),
            pltpu.VMEM((2, slots, pb), jnp.float32),
            pltpu.VMEM((slots, pb), jnp.float32),
            pltpu.VMEM((3, slots, pb), jnp.float32),
            pltpu.VMEM((slots, pb), jnp.float32),
            pltpu.VMEM((9, slots // N_CHUNK, pb), jnp.float32),
            pltpu.VMEM((tiles_all, 4 * TS, 2 * TS), jnp.float32),
            pltpu.VMEM((SKEW, 4 * TS, 2 * pb), jnp.float32),
            pltpu.VMEM((SKEW, 2 * TS, 2 * pb), jnp.float32),
            pltpu.SMEM((1, slots), jnp.int32),
            pltpu.VMEM((screen_size, tiles_all // (TILE_DEV * screen_size), 4 * TS, TILE_DEV * TS),
                       jnp.float32),
            pltpu.SemaphoreType.DMA((N_CHUNK, 5)),
            pltpu.SemaphoreType.DMA,
            pltpu.SemaphoreType.DMA((screen_size, tiles_all // (TILE_DEV * screen_size))),
        ],
        compiler_params=pltpu.CompilerParams(vmem_limit_bytes=60 * 1024 * 1024),
        name="deposit",
    )(block_count, place, block_tile, corner, offset, radius, emission, extinction)


def composite(stacked, slab_rank):
    slabs = stacked.shape[0]
    optical = stacked[:, 3 * TS:]
    glow = stacked[:, :3 * TS].reshape(slabs, 3, TS, TILE_DEV * TS)
    before = (slab_rank[None, :] < slab_rank[:, None]).astype(jnp.float32)
    prior = sum(before[:, k, None, None] * optical[k][None] for k in range(slabs))
    fade = jnp.exp(-prior) * jnp.exp(-0.5 * optical)
    light = jnp.sum(fade[:, None] * glow, axis=0).reshape(3 * TS, TILE_DEV * TS)
    cover = 1.0 - jnp.exp(-jnp.sum(optical, axis=0))
    image = jnp.concatenate([light, cover], axis=0)
    return image.reshape(4 * TS, TILE_DEV, TS).transpose(1, 2, 0)


def shards(block_tile, block_count, slab_rank, corner, offset, radius, emission, extinction):
    depth_size = lax.axis_size("depth")
    screen_size = lax.axis_size("screen")
    tiles_all = TILE_DEV * depth_size * screen_size
    me = lax.axis_index("screen")
    partial = deposit(block_tile, block_count, corner, offset, radius, emission, extinction,
                      tiles_all, me.astype(jnp.int32).reshape(1, 1), screen_size)
    owned = partial[0]
    moved = [
        lax.ppermute(partial[k], "screen", [(i, (i + k) % screen_size) for i in range(screen_size)])
        for k in range(1, screen_size)
    ]
    for block in moved:
        owned = owned + block
    dme = lax.axis_index("depth")
    pieces = [lax.dynamic_index_in_dim(owned, dme, 0, keepdims=True)]
    for k in range(1, depth_size):
        block = lax.dynamic_index_in_dim(owned, dme ^ k, 0, keepdims=True)
        pieces.append(lax.ppermute(block, "depth", [(i, i ^ k) for i in range(depth_size)]))
    slabs = jnp.concatenate(pieces, axis=0)
    slab_rank = slab_rank[dme ^ jnp.arange(depth_size)]
    return composite(slabs, slab_rank)


def solution(mesh):
    placed = (
        P("depth", "screen"),
        P("depth", "screen"),
        P(),
        P(None, "depth", "screen", None),
        P(None, "depth", "screen", None),
        P("depth", "screen", None),
        P(None, "depth", "screen", None),
        P("depth", "screen", None),
    )
    return jax.shard_map(
        shards,
        mesh=mesh,
        in_specs=placed,
        out_specs=P(("depth", "screen"), None, None),
        check_vma=False,
    )
```

```python
import functools

import jax
import jax.numpy as jnp
from jax import lax
from jax.experimental import pallas as pl
from jax.experimental.pallas import tpu as pltpu
from jax.sharding import PartitionSpec as P

TS = 32
FOOT = 16
TILE_DEV = 4
N_CHUNK = 16
UNROLL = 128
SKEW = 4


def deposit_kernel(tiles_all, slots, pb, screen_size, count_ref, place_ref, tile_hbm, corner_hbm,
                   offset_hbm, radius_hbm, emission_hbm, extinction_hbm, *rest):
    outs = rest[:screen_size]
    (corner_v, offset_v, radius_v, emission_v, extinction_v, prep, acc,
     late_lhs, late_rhs, tile_ref, ready, sems, tile_sem, out_sems) = rest[screen_size:]
    rows = slots // N_CHUNK
    live_count = count_ref[0, 0]

    def copies(chunk):
        sl = pl.ds(pl.multiple_of(chunk * rows, rows), rows)
        return [
            pltpu.make_async_copy(corner_hbm.at[:, 0, sl], corner_v.at[:, sl], sems.at[chunk, 0]),
            pltpu.make_async_copy(offset_hbm.at[:, 0, sl], offset_v.at[:, sl], sems.at[chunk, 1]),
            pltpu.make_async_copy(radius_hbm.at[0, sl], radius_v.at[sl], sems.at[chunk, 2]),
            pltpu.make_async_copy(emission_hbm.at[:, 0, sl], emission_v.at[:, sl], sems.at[chunk, 3]),
            pltpu.make_async_copy(extinction_hbm.at[0, sl], extinction_v.at[sl], sems.at[chunk, 4]),
        ]

    def start_chunk(chunk, carry):
        for copy in copies(chunk):
            copy.start()
        return carry

    lax.fori_loop(0, 2, start_chunk, 0)
    tile_copy = pltpu.make_async_copy(tile_hbm, tile_ref, tile_sem)
    tile_copy.start()

    def clear(t, carry):
        acc[t] = jnp.zeros((4 * TS, 2 * TS), jnp.float32)
        return carry

    lax.fori_loop(0, tiles_all, clear, 0)

    pixel = lax.broadcasted_iota(jnp.int32, (FOOT, pb), 0).astype(jnp.float32)
    unit = pixel / float(FOOT)

    def bump(edge, centre, h2):
        here = pixel >= edge
        s = jnp.where(here, unit, unit + 1.0) - centre
        p = jnp.maximum(h2 - s * s, 0.0)
        return here, p * p

    def laid_out(here, value):
        return jnp.concatenate([jnp.where(here, value, 0.0), jnp.where(here, 0.0, value)], axis=0)

    def with_rest(here, value):
        rest = value - value.astype(jnp.bfloat16).astype(jnp.float32)
        return laid_out(here, value), laid_out(here, rest)

    def factors(row):
        def param(k):
            return prep[k, pl.ds(row, 1), :]

        h2 = param(4)
        here_x, across = bump(param(0), param(1), h2)
        here_y, down = bump(param(2), param(3), h2)
        lhs = jnp.concatenate(
            [jnp.concatenate(with_rest(here_x, across * param(5 + c)), axis=1) for c in range(4)],
            axis=0)
        rhs = jnp.concatenate(
            [jnp.concatenate([part, part], axis=1) for part in with_rest(here_y, down)], axis=0)
        return lhs, rhs

    def product(lhs, rhs):
        return lax.dot_general(lhs, rhs, (((1,), (1,)), ((), ())),
                               preferred_element_type=jnp.float32)

    def add_late(base):
        for k in range(SKEW):
            t = tile_ref[0, jnp.maximum(base - SKEW + k, 0)]
            acc[t] = acc[t] + product(late_lhs[k], late_rhs[k])

    for k in range(SKEW):
        late_lhs[k] = jnp.zeros(late_lhs.shape[1:], jnp.float32)
        late_rhs[k] = jnp.zeros(late_rhs.shape[1:], jnp.float32)

    tile_copy.wait()

    def one_chunk(chunk, carry):
        for copy in copies(chunk):
            copy.wait()

        @pl.when(chunk + 2 < N_CHUNK)
        def _():
            start_chunk(chunk + 2, 0)

        first = pl.multiple_of(chunk * rows, rows)

        @pl.when(first < live_count)
        def _():
            sl = pl.ds(first, rows)
            for axis in range(2):
                edge = corner_v[axis, sl].astype(jnp.float32)
                prep[2 * axis] = edge
                prep[2 * axis + 1] = (edge - 0.5) / float(FOOT) + offset_v[axis, sl]
            unit_radius = radius_v[sl] / float(FOOT)
            h2 = unit_radius * unit_radius
            prep[4] = h2
            inv = 1.0 / h2
            inv = inv * inv
            slot_index = first + lax.broadcasted_iota(jnp.int32, (rows, pb), 0)
            scale = jnp.where(slot_index < live_count, inv * inv, 0.0)
            for c in range(3):
                prep[5 + c] = emission_v[c, sl] * scale
            prep[8] = extinction_v[sl] * scale
            live_here = jnp.minimum(live_count - first, rows)

            def one_group(group, inner):
                base = group * UNROLL
                late = [product(late_lhs[k], late_rhs[k]) for k in range(SKEW)]
                pairs = [factors(base + k) for k in range(UNROLL)]
                results = [product(*pair) for pair in pairs[:UNROLL - SKEW]]
                for k in range(SKEW):
                    late_lhs[k], late_rhs[k] = pairs[UNROLL - SKEW + k]
                for k, res in enumerate(late + results):
                    t = tile_ref[0, jnp.maximum(first + base - SKEW + k, 0)]
                    acc[t] = acc[t] + res
                return inner

            lax.fori_loop(0, (live_here + UNROLL - 1) // UNROLL, one_group, 0)

        return carry

    lax.fori_loop(0, N_CHUNK, one_chunk, 0)

    add_late((live_count + UNROLL - 1) // UNROLL * UNROLL)

    lane = lax.broadcasted_iota(jnp.int32, (4 * TS, TILE_DEV * TS), 1)
    even = (lane // TS) % 2 == 0

    def out_copy(k, d):
        return pltpu.make_async_copy(ready.at[k, d], outs[k].at[d], out_sems.at[k, d])

    def finish(d, carry):
        for k in range(screen_size):
            s = lax.rem(place_ref[0, 0] + k, screen_size)
            tile = (d * screen_size + s) * TILE_DEV
            wide = [jnp.concatenate([acc[tile + q], acc[tile + q + 2]], axis=1) for q in range(2)]
            turned = [pltpu.roll(wide[0], 3 * TS, axis=1), pltpu.roll(wide[1], TS, axis=1)]
            ready[k, d] = jnp.where(even, wide[0] + turned[0], wide[1] + turned[1])
            out_copy(k, d).start()
        return carry

    lax.fori_loop(0, tiles_all // (TILE_DEV * screen_size), finish, 0)

    def drain(d, carry):
        for k in range(screen_size):
            out_copy(k, d).wait()
        return carry

    lax.fori_loop(0, tiles_all // (TILE_DEV * screen_size), drain, 0)


def deposit(block_tile, block_count, corner, offset, radius, emission, extinction, tiles_all,
            place, screen_size):
    slots, pb = radius.shape[1:]
    any_space = pl.BlockSpec(memory_space=pl.ANY)
    smem = pl.BlockSpec(memory_space=pltpu.SMEM)
    return pl.pallas_call(
        functools.partial(deposit_kernel, tiles_all, slots, pb, screen_size),
        out_shape=[jax.ShapeDtypeStruct(
            (tiles_all // (TILE_DEV * screen_size), 4 * TS, TILE_DEV * TS), jnp.float32)
        ] * screen_size,
        in_specs=[smem, smem] + [any_space] * 6,
        out_specs=[any_space] * screen_size,
        scratch_shapes=[
            pltpu.VMEM((2, slots, pb), jnp.int32),
            pltpu.VMEM((2, slots, pb), jnp.float32),
            pltpu.VMEM((slots, pb), jnp.float32),
            pltpu.VMEM((3, slots, pb), jnp.float32),
            pltpu.VMEM((slots, pb), jnp.float32),
            pltpu.VMEM((9, slots // N_CHUNK, pb), jnp.float32),
            pltpu.VMEM((tiles_all, 4 * TS, 2 * TS), jnp.float32),
            pltpu.VMEM((SKEW, 4 * TS, 2 * pb), jnp.float32),
            pltpu.VMEM((SKEW, 2 * TS, 2 * pb), jnp.float32),
            pltpu.SMEM((1, slots), jnp.int32),
            pltpu.VMEM((screen_size, tiles_all // (TILE_DEV * screen_size), 4 * TS, TILE_DEV * TS),
                       jnp.float32),
            pltpu.SemaphoreType.DMA((N_CHUNK, 5)),
            pltpu.SemaphoreType.DMA,
            pltpu.SemaphoreType.DMA((screen_size, tiles_all // (TILE_DEV * screen_size))),
        ],
        compiler_params=pltpu.CompilerParams(vmem_limit_bytes=60 * 1024 * 1024),
        name="deposit",
    )(block_count, place, block_tile, corner, offset, radius, emission, extinction)


def composite(stacked, slab_rank):
    slabs = stacked.shape[0]
    optical = stacked[:, 3 * TS:]
    glow = stacked[:, :3 * TS].reshape(slabs, 3, TS, TILE_DEV * TS)
    before = (slab_rank[None, :] < slab_rank[:, None]).astype(jnp.float32)
    prior = sum(before[:, k, None, None] * optical[k][None] for k in range(slabs))
    fade = jnp.exp(-prior) * jnp.exp(-0.5 * optical)
    light = jnp.sum(fade[:, None] * glow, axis=0).reshape(3 * TS, TILE_DEV * TS)
    cover = 1.0 - jnp.exp(-jnp.sum(optical, axis=0))
    image = jnp.concatenate([light, cover], axis=0)
    return image.reshape(4 * TS, TILE_DEV, TS).transpose(1, 2, 0)


def shards(block_tile, block_count, slab_rank, corner, offset, radius, emission, extinction):
    depth_size = lax.axis_size("depth")
    screen_size = lax.axis_size("screen")
    tiles_all = TILE_DEV * depth_size * screen_size
    me = lax.axis_index("screen")
    partial = deposit(block_tile, block_count, corner, offset, radius, emission, extinction,
                      tiles_all, me.astype(jnp.int32).reshape(1, 1), screen_size)
    owned = partial[0]
    moved = [
        lax.ppermute(partial[k], "screen", [(i, (i + k) % screen_size) for i in range(screen_size)])
        for k in range(1, screen_size)
    ]
    for block in moved:
        owned = owned + block
    dme = lax.axis_index("depth")
    pieces = [lax.dynamic_index_in_dim(owned, dme, 0, keepdims=True)]
    for k in range(1, depth_size):
        block = lax.dynamic_index_in_dim(owned, dme ^ k, 0, keepdims=True)
        pieces.append(lax.ppermute(block, "depth", [(i, i ^ k) for i in range(depth_size)]))
    slabs = jnp.concatenate(pieces, axis=0)
    slab_rank = slab_rank[dme ^ jnp.arange(depth_size)]
    return composite(slabs, slab_rank)


def solution(mesh):
    placed = (
        P("depth", "screen"),
        P("depth", "screen"),
        P(),
        P(None, "depth", "screen", None),
        P(None, "depth", "screen", None),
        P("depth", "screen", None),
        P(None, "depth", "screen", None),
        P("depth", "screen", None),
    )
    return jax.shard_map(
        shards,
        mesh=mesh,
        in_specs=placed,
        out_specs=P(("depth", "screen"), None, None),
        check_vma=False,
    )
```

```python
import functools

import jax
import jax.numpy as jnp
from jax import lax
from jax.experimental import pallas as pl
from jax.experimental.pallas import tpu as pltpu
from jax.sharding import PartitionSpec as P

TS = 32
FOOT = 16
TILE_DEV = 4
N_CHUNK = 8
UNROLL = 256
SKEW = 4


def deposit_kernel(tiles_all, slots, pb, screen_size, count_ref, place_ref, tile_hbm, corner_hbm,
                   offset_hbm, radius_hbm, emission_hbm, extinction_hbm, *rest):
    outs = rest[:screen_size]
    (corner_v, offset_v, radius_v, emission_v, extinction_v, prep, acc,
     late_lhs, late_rhs, tile_ref, ready, sems, tile_sem, out_sems) = rest[screen_size:]
    rows = slots // N_CHUNK
    live_count = count_ref[0, 0]

    def copies(chunk):
        sl = pl.ds(pl.multiple_of(chunk * rows, rows), rows)
        return [
            pltpu.make_async_copy(corner_hbm.at[:, 0, sl], corner_v.at[:, sl], sems.at[chunk, 0]),
            pltpu.make_async_copy(offset_hbm.at[:, 0, sl], offset_v.at[:, sl], sems.at[chunk, 1]),
            pltpu.make_async_copy(radius_hbm.at[0, sl], radius_v.at[sl], sems.at[chunk, 2]),
            pltpu.make_async_copy(emission_hbm.at[:, 0, sl], emission_v.at[:, sl], sems.at[chunk, 3]),
            pltpu.make_async_copy(extinction_hbm.at[0, sl], extinction_v.at[sl], sems.at[chunk, 4]),
        ]

    def start_chunk(chunk, carry):
        for copy in copies(chunk):
            copy.start()
        return carry

    lax.fori_loop(0, 2, start_chunk, 0)
    tile_copy = pltpu.make_async_copy(tile_hbm, tile_ref, tile_sem)
    tile_copy.start()

    def clear(t, carry):
        acc[t] = jnp.zeros((4 * TS, 2 * TS), jnp.float32)
        return carry

    lax.fori_loop(0, tiles_all, clear, 0)

    pixel = lax.broadcasted_iota(jnp.int32, (FOOT, pb), 0).astype(jnp.float32)
    unit = pixel / float(FOOT)

    def bump(edge, centre, h2):
        here = pixel >= edge
        s = jnp.where(here, unit, unit + 1.0) - centre
        p = jnp.maximum(h2 - s * s, 0.0)
        return here, p * p

    def laid_out(here, value):
        return jnp.concatenate([jnp.where(here, value, 0.0), jnp.where(here, 0.0, value)], axis=0)

    def with_rest(here, value):
        rest = value - value.astype(jnp.bfloat16).astype(jnp.float32)
        return laid_out(here, value), laid_out(here, rest)

    def factors(row):
        def param(k):
            return prep[k, pl.ds(row, 1), :]

        h2 = param(4)
        here_x, across = bump(param(0), param(1), h2)
        here_y, down = bump(param(2), param(3), h2)
        lhs = jnp.concatenate(
            [jnp.concatenate(with_rest(here_x, across * param(5 + c)), axis=1) for c in range(4)],
            axis=0)
        rhs = jnp.concatenate(
            [jnp.concatenate([part, part], axis=1) for part in with_rest(here_y, down)], axis=0)
        return lhs, rhs

    def product(lhs, rhs):
        return lax.dot_general(lhs, rhs, (((1,), (1,)), ((), ())),
                               preferred_element_type=jnp.float32)

    def add_late(base):
        for k in range(SKEW):
            t = tile_ref[0, jnp.maximum(base - SKEW + k, 0)]
            acc[t] = acc[t] + product(late_lhs[k], late_rhs[k])

    for k in range(SKEW):
        late_lhs[k] = jnp.zeros(late_lhs.shape[1:], jnp.float32)
        late_rhs[k] = jnp.zeros(late_rhs.shape[1:], jnp.float32)

    tile_copy.wait()

    def one_chunk(chunk, carry):
        for copy in copies(chunk):
            copy.wait()

        @pl.when(chunk + 2 < N_CHUNK)
        def _():
            start_chunk(chunk + 2, 0)

        first = pl.multiple_of(chunk * rows, rows)

        @pl.when(first < live_count)
        def _():
            sl = pl.ds(first, rows)
            for axis in range(2):
                edge = corner_v[axis, sl].astype(jnp.float32)
                prep[2 * axis] = edge
                prep[2 * axis + 1] = (edge - 0.5) / float(FOOT) + offset_v[axis, sl]
            unit_radius = radius_v[sl] / float(FOOT)
            h2 = unit_radius * unit_radius
            prep[4] = h2
            inv = 1.0 / h2
            inv = inv * inv
            slot_index = first + lax.broadcasted_iota(jnp.int32, (rows, pb), 0)
            scale = jnp.where(slot_index < live_count, inv * inv, 0.0)
            for c in range(3):
                prep[5 + c] = emission_v[c, sl] * scale
            prep[8] = extinction_v[sl] * scale
            live_here = jnp.minimum(live_count - first, rows)

            def one_group(group, inner):
                base = group * UNROLL
                late = [product(late_lhs[k], late_rhs[k]) for k in range(SKEW)]
                pairs = [factors(base + k) for k in range(UNROLL)]
                results = [product(*pair) for pair in pairs[:UNROLL - SKEW]]
                for k in range(SKEW):
                    late_lhs[k], late_rhs[k] = pairs[UNROLL - SKEW + k]
                for k, res in enumerate(late + results):
                    t = tile_ref[0, jnp.maximum(first + base - SKEW + k, 0)]
                    acc[t] = acc[t] + res
                return inner

            lax.fori_loop(0, (live_here + UNROLL - 1) // UNROLL, one_group, 0)

        return carry

    lax.fori_loop(0, N_CHUNK, one_chunk, 0)

    add_late((live_count + UNROLL - 1) // UNROLL * UNROLL)

    lane = lax.broadcasted_iota(jnp.int32, (4 * TS, TILE_DEV * TS), 1)
    even = (lane // TS) % 2 == 0

    def out_copy(k, d):
        return pltpu.make_async_copy(ready.at[k, d], outs[k].at[d], out_sems.at[k, d])

    def finish(d, carry):
        for k in range(screen_size):
            s = lax.rem(place_ref[0, 0] + k, screen_size)
            tile = (d * screen_size + s) * TILE_DEV
            wide = [jnp.concatenate([acc[tile + q], acc[tile + q + 2]], axis=1) for q in range(2)]
            turned = [pltpu.roll(wide[0], 3 * TS, axis=1), pltpu.roll(wide[1], TS, axis=1)]
            ready[k, d] = jnp.where(even, wide[0] + turned[0], wide[1] + turned[1])
            out_copy(k, d).start()
        return carry

    lax.fori_loop(0, tiles_all // (TILE_DEV * screen_size), finish, 0)

    def drain(d, carry):
        for k in range(screen_size):
            out_copy(k, d).wait()
        return carry

    lax.fori_loop(0, tiles_all // (TILE_DEV * screen_size), drain, 0)


def deposit(block_tile, block_count, corner, offset, radius, emission, extinction, tiles_all,
            place, screen_size):
    slots, pb = radius.shape[1:]
    any_space = pl.BlockSpec(memory_space=pl.ANY)
    smem = pl.BlockSpec(memory_space=pltpu.SMEM)
    return pl.pallas_call(
        functools.partial(deposit_kernel, tiles_all, slots, pb, screen_size),
        out_shape=[jax.ShapeDtypeStruct(
            (tiles_all // (TILE_DEV * screen_size), 4 * TS, TILE_DEV * TS), jnp.float32)
        ] * screen_size,
        in_specs=[smem, smem] + [any_space] * 6,
        out_specs=[any_space] * screen_size,
        scratch_shapes=[
            pltpu.VMEM((2, slots, pb), jnp.int32),
            pltpu.VMEM((2, slots, pb), jnp.float32),
            pltpu.VMEM((slots, pb), jnp.float32),
            pltpu.VMEM((3, slots, pb), jnp.float32),
            pltpu.VMEM((slots, pb), jnp.float32),
            pltpu.VMEM((9, slots // N_CHUNK, pb), jnp.float32),
            pltpu.VMEM((tiles_all, 4 * TS, 2 * TS), jnp.float32),
            pltpu.VMEM((SKEW, 4 * TS, 2 * pb), jnp.float32),
            pltpu.VMEM((SKEW, 2 * TS, 2 * pb), jnp.float32),
            pltpu.SMEM((1, slots), jnp.int32),
            pltpu.VMEM((screen_size, tiles_all // (TILE_DEV * screen_size), 4 * TS, TILE_DEV * TS),
                       jnp.float32),
            pltpu.SemaphoreType.DMA((N_CHUNK, 5)),
            pltpu.SemaphoreType.DMA,
            pltpu.SemaphoreType.DMA((screen_size, tiles_all // (TILE_DEV * screen_size))),
        ],
        compiler_params=pltpu.CompilerParams(vmem_limit_bytes=60 * 1024 * 1024),
        name="deposit",
    )(block_count, place, block_tile, corner, offset, radius, emission, extinction)


def composite(stacked, slab_rank):
    slabs = stacked.shape[0]
    optical = stacked[:, 3 * TS:]
    glow = stacked[:, :3 * TS].reshape(slabs, 3, TS, TILE_DEV * TS)
    before = (slab_rank[None, :] < slab_rank[:, None]).astype(jnp.float32)
    prior = sum(before[:, k, None, None] * optical[k][None] for k in range(slabs))
    fade = jnp.exp(-prior) * jnp.exp(-0.5 * optical)
    light = jnp.sum(fade[:, None] * glow, axis=0).reshape(3 * TS, TILE_DEV * TS)
    cover = 1.0 - jnp.exp(-jnp.sum(optical, axis=0))
    image = jnp.concatenate([light, cover], axis=0)
    return image.reshape(4 * TS, TILE_DEV, TS).transpose(1, 2, 0)


def shards(block_tile, block_count, slab_rank, corner, offset, radius, emission, extinction):
    depth_size = lax.axis_size("depth")
    screen_size = lax.axis_size("screen")
    tiles_all = TILE_DEV * depth_size * screen_size
    me = lax.axis_index("screen")
    partial = deposit(block_tile, block_count, corner, offset, radius, emission, extinction,
                      tiles_all, me.astype(jnp.int32).reshape(1, 1), screen_size)
    owned = partial[0]
    moved = [
        lax.ppermute(partial[k], "screen", [(i, (i + k) % screen_size) for i in range(screen_size)])
        for k in range(1, screen_size)
    ]
    for block in moved:
        owned = owned + block
    dme = lax.axis_index("depth")
    pieces = [lax.dynamic_index_in_dim(owned, dme, 0, keepdims=True)]
    for k in range(1, depth_size):
        block = lax.dynamic_index_in_dim(owned, dme ^ k, 0, keepdims=True)
        pieces.append(lax.ppermute(block, "depth", [(i, i ^ k) for i in range(depth_size)]))
    slabs = jnp.concatenate(pieces, axis=0)
    slab_rank = slab_rank[dme ^ jnp.arange(depth_size)]
    return composite(slabs, slab_rank)


def solution(mesh):
    placed = (
        P("depth", "screen"),
        P("depth", "screen"),
        P(),
        P(None, "depth", "screen", None),
        P(None, "depth", "screen", None),
        P("depth", "screen", None),
        P(None, "depth", "screen", None),
        P("depth", "screen", None),
    )
    return jax.shard_map(
        shards,
        mesh=mesh,
        in_specs=placed,
        out_specs=P(("depth", "screen"), None, None),
        check_vma=False,
    )
```
